256 devices in a mesh: row: 16 (over y_lo, x, core), col: 16 (over z, y_hi).
Axes of the slice: x: 4, y: 4 (y_hi: 2, y_lo: 2; y = y_hi * 2 + y_lo), z: 8, core: 2. Of those that a mesh axis runs over, the one named last changes fastest.
Arguments:
- tokens: bfloat16 [16, 16, 736, 1024], P('row', 'col'), may hold values from -6 to 6
- local_params: bfloat16 [16, 16, 2, 1024, 1024], P('row', 'col'), may hold values from -0.1875 to 0.1875
- outer_params: float32 [2, 16, 16, 16, 4, 1024], P(None, None, 'col', 'row'), may hold values from -0.1875 to 0.1875
- momentum: float32 [2, 16, 16, 16, 4, 1024], P(None, None, 'col', 'row'), may hold values from -0.1875 to 0.1875
- table: int32 [16, 16], replicated, may hold values from 0 to 15, each once within a row
- counts: int32 [16, 16], replicated, may hold values from 64 to 4095
Outputs:
- path_params: bfloat16 [16, 16, 2, 1024, 1024], P('row', 'col')
- outer_out: float32 [2, 16, 16, 16, 4, 1024], P(None, None, 'col', 'row')
- momentum_out: float32 [2, 16, 16, 16, 4, 1024], P(None, None, 'col', 'row')
- hidden_out: bfloat16 [16, 16, 736, 1024], P('row', 'col')
The draws below stay inside these ranges and needn't reach their ends.
Inputs may be any that keep to these rules, and one draw needn't show every extreme that they name: Each row of the table names every level-two module exactly once.
All inputs are finite; a program needn't handle non-finite values.
Results may differ from the reference program's by a relative error of at most 0.01.
Values may be sent and summed in bfloat16 or wider, within the bound.
No kernel may reach another device: no remote copies, remote signals or barrier semaphores. Data moves between devices by JAX's collectives and lax.ppermute only.
A program may use at most 64 MiB of HBM per device.

```python
import jax
import jax.numpy as jnp
from jax import lax

D = 1024
LAYERS = 2
TOK_DEV = 736
MODULES = 16
ROWS_PIECE = 4
N_ROW = 16
N_COL = 16


def place_ends(entries, stream_key, smallest, largest):
    shape = entries.shape
    index_at = [jax.random.randint(jax.random.fold_in(stream_key, axis), (), 0, shape[axis]) for axis in range(len(shape))]
    entries = entries.at[tuple(index_at)].set(smallest)
    longest = shape.index(max(shape))
    index_at[longest] = (index_at[longest] + 1) % shape[longest]
    return entries.at[tuple(index_at)].set(largest)


def block_levels(rng, extent, split, smallest, high):
    loudness = 1.0
    for position, blocks in split:
        heights = jax.random.uniform(jax.random.fold_in(jax.random.fold_in(rng, 6), position), (blocks,), jnp.float32, smallest / len(split), high / len(split))
        loudness = loudness * jnp.repeat(jnp.exp(heights), extent[position] // blocks).reshape((-1,) + (1,) * (len(extent) - 1 - position))
    return loudness


def bell_draw(key, dims, scale, most, cuts=(), held_as=jnp.bfloat16):
    result = jax.random.normal(key, dims, jnp.float32) * scale
    if len(cuts) > 0:
        result = block_levels(key, dims, cuts, -0.22, 0.18) * result
    return jnp.clip(result, min=-most, max=most).astype(held_as)


def setup_inputs(seed: int = 0) -> dict:
    key_list = jax.random.split(jax.random.key(seed), 7)
    return {
        "tokens": bell_draw(key_list[0], (N_ROW, N_COL, TOK_DEV, D), 1.0, 6.0, ((0, 16), (1, 16))),
        "local_params": bell_draw(key_list[1], (N_ROW, N_COL, LAYERS, D, D), D ** -0.5, 0.1875, ((0, 16), (1, 16))),
        "outer_params": bell_draw(key_list[2], (LAYERS, MODULES, N_COL, N_ROW, ROWS_PIECE, D), D ** -0.5, 0.1875, ((2, 16), (3, 16)), jnp.float32),
        "momentum": bell_draw(key_list[3], (LAYERS, MODULES, N_COL, N_ROW, ROWS_PIECE, D), D ** -0.5, 0.1875, ((2, 16), (3, 16)), jnp.float32),
        "table": jax.vmap(lambda own: jax.random.permutation(own, N_COL))(jax.random.split(key_list[4], N_ROW)).reshape((N_ROW, N_COL)).astype(jnp.int32),
        "counts": place_ends(jax.random.randint(key_list[5], (N_ROW, N_COL), 64, 4096), jax.random.fold_in(key_list[5], 1), 64, 4095).astype(jnp.int32),
    }


def micro_step(tokens_path, params_path):
    state = tokens_path.astype(jnp.float32)
    for layer in range(LAYERS):
        scale = lax.rsqrt(lax.optimization_barrier(jnp.mean(state * state, axis=-1, keepdims=True)) + 1e-06)
        normed = (state * scale).astype(jnp.bfloat16)
        mixed = jnp.dot(normed, params_path[layer], preferred_element_type=jnp.float32)
        state = state + jax.nn.gelu(mixed, approximate=False)
    return state.astype(jnp.bfloat16)

def reference(tokens, local_params, outer_params, momentum, table, counts):
    n_row = table.shape[0]
    n_col = table.shape[1]
    width = local_params.shape[-1]
    layers = local_params.shape[2]
    ids = jnp.arange(n_col, dtype=jnp.int32)
    matches = (table[:, :, None] == ids[None, None, :]).astype(jnp.float32)
    totals = lax.optimization_barrier(jnp.sum(counts.astype(jnp.float32)[:, :, None] * matches, axis=(0, 1)))
    share = counts.astype(jnp.float32) / lax.optimization_barrier(jnp.sum(matches * totals[None, None, :], axis=2))
    slots = jnp.arange(n_col, dtype=jnp.int32)
    inverse = lax.optimization_barrier(jnp.sum(slots[None, :, None] * (table[:, :, None] == ids[None, None, :]).astype(jnp.int32), axis=1)).astype(jnp.int32)

    def add_row(acc, index):
        local_row = local_params[index]
        weights = share[index]
        term = (weights[:, None, None, None] * local_row.astype(jnp.float32)).astype(jnp.bfloat16)
        ordered = jnp.take(term, inverse[index], axis=0)
        return (acc + jnp.transpose(ordered.astype(jnp.float32), (1, 0, 2, 3)), None)
    start = jnp.zeros((layers, n_col, width, width), jnp.float32)
    average, unused = lax.scan(add_row, start, jnp.arange(n_row, dtype=jnp.int32))
    outer = outer_params.reshape(layers, n_col, width, width)
    moment = momentum.reshape(layers, n_col, width, width)
    delta = outer - average
    moment_new = 0.9 * moment + delta
    outer_new = outer - 0.7 * (delta + 0.9 * moment_new)
    picked = jnp.take(outer_new.astype(jnp.bfloat16), table, axis=1)
    path_params = jnp.transpose(picked, (1, 2, 0, 3, 4))
    flat_tokens = tokens.reshape(n_row * n_col, tokens.shape[2], width)
    flat_params = local_params.reshape(n_row * n_col, layers, width, width)
    hidden = lax.map(lambda pair: micro_step(pair[0], pair[1]), (flat_tokens, flat_params))
    hidden_out = hidden.reshape(tokens.shape)
    return (path_params, outer_new.reshape(outer_params.shape), moment_new.reshape(momentum.shape), hidden_out)
```

```python
import functools

import jax
import jax.numpy as jnp
from jax import lax
from jax.experimental import pallas as pl
from jax.experimental.pallas import tpu as pltpu
from jax.sharding import Mesh
from jax.sharding import PartitionSpec as P

N_CHUNK = 1
PLANE = ("yl", "x", "core", "yh")
F32 = jnp.float32
BF16 = jnp.bfloat16


def cost(flops, bytes_accessed):
    return pl.CostEstimate(flops=flops, bytes_accessed=bytes_accessed, transcendentals=0)


def low_half(shape):
    return lax.broadcasted_iota(jnp.int32, shape, len(shape) - 2) < 4


def swap_halves(first, second):
    mask = low_half(first.shape)
    axis = len(first.shape) - 2
    return (
        jnp.where(mask, first, pltpu.roll(second, 4, axis)),
        jnp.where(mask, pltpu.roll(first, 4, axis), second),
    )


def pack_kernel(place, table, counts, params, *outs):
    ids = table[...]
    tokens = counts[...].astype(F32)
    here = (lax.broadcasted_iota(jnp.int32, ids.shape, 0) == place[0]) & (
        lax.broadcasted_iota(jnp.int32, ids.shape, 1) == place[1]
    )
    module = jnp.sum(jnp.where(here, ids, 0).astype(F32))
    total = jnp.sum(jnp.where(ids.astype(F32) == module, tokens, 0.0), keepdims=True)
    mine = jnp.sum(jnp.where(here, tokens, 0.0), keepdims=True)
    share = mine / total
    width = params.shape[-1] // len(outs)
    for yh in range(2):
        for pair in range(8):
            rows = pl.ds(yh * 64 + pair * 8, 8)
            for h, out in enumerate(outs):
                cols = pl.ds(h * width, width)
                first = params[0, 0, rows, cols].astype(F32) * share
                second = params[1, 0, rows, cols].astype(F32) * share
                even, odd = swap_halves(first, second)
                out[(2 * pair) * 2 + yh, 0] = even.astype(BF16)
                out[(2 * pair + 1) * 2 + yh, 0] = odd.astype(BF16)


def pack(place, table, counts, params):
    layers, width = params.shape[0], params.shape[-1]
    view = params.reshape(layers, 8, 128, width)
    part = width // N_CHUNK
    return pl.pallas_call(
        pack_kernel,
        name="pack",
        grid_spec=pltpu.PrefetchScalarGridSpec(
            num_scalar_prefetch=1,
            grid=(8,),
            in_specs=[
                pl.BlockSpec((16, 16), lambda z, s: (0, 0)),
                pl.BlockSpec((16, 16), lambda z, s: (0, 0)),
                pl.BlockSpec((layers, 1, 128, width), lambda z, s: (0, z, 0, 0)),
            ],
            out_specs=[pl.BlockSpec((32, 1, 8, part), lambda z, s: (0, z, 0, 0))] * N_CHUNK,
        ),
        out_shape=[jax.ShapeDtypeStruct((32, 8, 8, part), BF16)] * N_CHUNK,
        cost_estimate=cost(2 * view.size, 4 * view.size),
    )(place, table, counts, view)


def combine_kernel(mods, arrived, out, acc):
    acc[...] = jnp.zeros_like(acc)
    for s in range(arrived.shape[0]):
        acc[mods[s]] += arrived[s, 0].astype(F32)
    out[0] = acc[...].astype(BF16)


def combine(mods, arrived):
    n, nz, rows, width = arrived.shape
    return pl.pallas_call(
        combine_kernel,
        name="combine",
        grid_spec=pltpu.PrefetchScalarGridSpec(
            num_scalar_prefetch=1,
            grid=(nz,),
            in_specs=[pl.BlockSpec((n, 1, rows, width), lambda z, s: (0, z, 0, 0))],
            out_specs=pl.BlockSpec((1, 16, rows, width), lambda z, s: (z, 0, 0, 0)),
            scratch_shapes=[pltpu.VMEM((16, rows, width), F32)],
        ),
        out_shape=jax.ShapeDtypeStruct((nz, 16, rows, width), BF16),
        cost_estimate=cost(arrived.size, 3 * arrived.size),
    )(mods, arrived)


def update_kernel(n, *refs):
    sums, outer, moment = refs[:n], refs[n], refs[n + 1]
    outer_out, moment_out, news = refs[n + 2], refs[n + 3], refs[n + 4 :]
    width = outer.shape[-1] // n
    for h in range(n):
        cols = pl.ds(h * width, width)
        for m in range(16):
            average = sums[h][m].astype(F32)
            parts = []
            for layer in range(2):
                old = outer[layer, m, :, cols]
                delta = old - average[layer * 4 : layer * 4 + 4]
                moved = 0.9 * moment[layer, m, :, cols] + delta
                new = old - 0.7 * (delta + 0.9 * moved)
                outer_out[layer, m, :, cols] = new
                moment_out[layer, m, :, cols] = moved
                parts.append(new)
            news[h][m] = jnp.concatenate(parts, axis=0).astype(BF16)


def update(sums, outer, moment):
    n = len(sums)
    vmem = pl.BlockSpec(memory_space=pltpu.VMEM)
    got = pl.pallas_call(
        functools.partial(update_kernel, n),
        name="update",
        in_specs=[vmem] * (n + 2),
        out_specs=[vmem] * (n + 2),
        out_shape=[jax.ShapeDtypeStruct(outer.shape, F32)] * 2
        + [jax.ShapeDtypeStruct(s.shape, BF16) for s in sums],
        cost_estimate=cost(8 * outer.size, 20 * outer.size),
    )(*sums, outer, moment)
    return got[0], got[1], got[2:]


def choose_kernel(mods, whole, out):
    for d in range(out.shape[0]):
        out[d, 0] = whole[0, mods[d]]


def choose(mods, whole):
    nz, _, rows, width = whole.shape
    return pl.pallas_call(
        choose_kernel,
        name="choose",
        grid_spec=pltpu.PrefetchScalarGridSpec(
            num_scalar_prefetch=1,
            grid=(nz,),
            in_specs=[pl.BlockSpec((1, 16, rows, width), lambda z, s: (z, 0, 0, 0))],
            out_specs=pl.BlockSpec((32, 1, rows, width), lambda z, s: (0, z, 0, 0)),
        ),
        out_shape=jax.ShapeDtypeStruct((32, nz, rows, width), BF16),
        cost_estimate=cost(0, 6 * whole.size),
    )(mods, whole)


def unpack_kernel(*refs):
    got, out = refs[:-1], refs[-1]
    width = out.shape[-1] // len(got)
    for yh in range(2):
        for pair in range(8):
            rows = pl.ds(yh * 64 + pair * 8, 8)
            for h, ref in enumerate(got):
                cols = pl.ds(h * width, width)
                even = ref[(2 * pair) * 2 + yh, 0].astype(F32)
                odd = ref[(2 * pair + 1) * 2 + yh, 0].astype(F32)
                first, second = swap_halves(even, odd)
                out[0, 0, rows, cols] = first.astype(BF16)
                out[1, 0, rows, cols] = second.astype(BF16)


def unpack(got, width):
    part = got[0].shape[-1]
    return pl.pallas_call(
        unpack_kernel,
        name="unpack",
        grid=(8,),
        in_specs=[pl.BlockSpec((32, 1, 8, part), lambda z: (0, z, 0, 0))] * len(got),
        out_specs=pl.BlockSpec((2, 1, 128, width), lambda z: (0, z, 0, 0)),
        out_shape=jax.ShapeDtypeStruct((2, 8, 128, width), BF16),
        cost_estimate=cost(0, 8 * width * width),
    )(*got).reshape(2, 1024, width)


def micro_step(tokens_path, params_path):
    state = tokens_path.astype(F32)
    for layer in range(params_path.shape[0]):
        scale = lax.rsqrt(jnp.mean(state * state, axis=-1, keepdims=True) + 1e-06)
        normed = (state * scale).astype(BF16)
        mixed = jnp.dot(normed, params_path[layer], preferred_element_type=F32)
        state = state + jax.nn.gelu(mixed, approximate=False)
    return state.astype(BF16)


def in_plane(blocks):
    return lax.all_to_all(blocks, PLANE, split_axis=0, concat_axis=0, tiled=True)


def on_device(tokens, local_params, outer_params, momentum, table, counts):
    row = lax.axis_index(("yl", "x", "core")).astype(jnp.int32)
    z = lax.axis_index("z").astype(jnp.int32)
    col = z * 2 + lax.axis_index("yh").astype(jnp.int32)
    place = jnp.stack([row, col])
    mods = lax.dynamic_slice(table, (0, z * 2), (16, 2)).reshape(32)
    params = local_params[0, 0]
    width = params.shape[-1]
    outer = outer_params.reshape(2, 16, 4, width)
    moment = momentum.reshape(2, 16, 4, width)
    packed = pack(place, table, counts, params)
    hidden = micro_step(tokens[0, 0], params)
    sums = []
    for chunk in packed:
        dense = combine(mods, in_plane(chunk))
        part = lax.psum_scatter(dense, "z", scatter_dimension=0, tiled=True)
        sums.append(part[0])
    outer_new, moment_new, news = update(sums, outer, moment)
    got = []
    for new in news:
        whole = lax.all_gather(new, "z", axis=0)
        got.append(in_plane(choose(mods, whole)))
    returned = unpack(got, width)
    return (
        returned[None, None],
        outer_new.reshape(outer_params.shape),
        moment_new.reshape(momentum.shape),
        hidden[None, None],
    )


def solution(mesh):
    devices = mesh.devices.reshape(2, 4, 2, 8, 2)
    fine = Mesh(devices, ("yl", "x", "core", "z", "yh"))
    row, col = ("yl", "x", "core"), ("z", "yh")
    return jax.shard_map(
        on_device,
        mesh=fine,
        in_specs=(
            P(row, col, None, None),
            P(row, col, None, None, None),
            P(None, None, col, row, None, None),
            P(None, None, col, row, None, None),
            P(),
            P(),
        ),
        out_specs=(
            P(row, col, None, None, None),
            P(None, None, col, row, None, None),
            P(None, None, col, row, None, None),
            P(row, col, None, None),
        ),
        check_vma=False,
    )
```

```python
import functools

import jax
import jax.numpy as jnp
from jax import lax
from jax.experimental import pallas as pl
from jax.experimental.pallas import tpu as pltpu
from jax.sharding import Mesh
from jax.sharding import PartitionSpec as P

N_CHUNK = 2
PLANE = ("yl", "x", "core", "zl", "yh")
F32 = jnp.float32
BF16 = jnp.bfloat16


def cost(flops, bytes_accessed):
    return pl.CostEstimate(flops=flops, bytes_accessed=bytes_accessed, transcendentals=0)


def low_half(shape):
    return lax.broadcasted_iota(jnp.int32, shape, len(shape) - 2) < 4


def swap_halves(first, second):
    mask = low_half(first.shape)
    axis = len(first.shape) - 2
    return (
        jnp.where(mask, first, pltpu.roll(second, 4, axis)),
        jnp.where(mask, pltpu.roll(first, 4, axis), second),
    )


def pack_kernel(place, table, counts, params, out):
    ids = table[...]
    tokens = counts[...].astype(F32)
    here = (lax.broadcasted_iota(jnp.int32, ids.shape, 0) == place[0]) & (
        lax.broadcasted_iota(jnp.int32, ids.shape, 1) == place[1]
    )
    module = jnp.sum(jnp.where(here, ids, 0).astype(F32))
    total = jnp.sum(jnp.where(ids.astype(F32) == module, tokens, 0.0), keepdims=True)
    mine = jnp.sum(jnp.where(here, tokens, 0.0), keepdims=True)
    share = mine / total
    for yh in range(2):
        for pair in range(8):
            rows = pl.ds(yh * 64 + pair * 8, 8)
            first = params[0, 0, rows].astype(F32) * share
            second = params[1, 0, rows].astype(F32) * share
            even, odd = swap_halves(first, second)
            out[2 * pair, 0, yh, 0] = even.astype(BF16)
            out[2 * pair + 1, 0, yh, 0] = odd.astype(BF16)


def pack(h, place, table, counts, params):
    layers, width = params.shape[0], params.shape[-1]
    view = params.reshape(layers, 8, 128, width)
    part = width // N_CHUNK
    return pl.pallas_call(
        pack_kernel,
        name=f"pack{h}",
        grid_spec=pltpu.PrefetchScalarGridSpec(
            num_scalar_prefetch=1,
            grid=(8,),
            in_specs=[
                pl.BlockSpec((16, 16), lambda z, s: (0, 0)),
                pl.BlockSpec((16, 16), lambda z, s: (0, 0)),
                pl.BlockSpec((layers, 1, 128, part), lambda z, s: (0, z, 0, h)),
            ],
            out_specs=pl.BlockSpec((16, 1, 2, 1, 8, part), lambda z, s: (0, z % 2, 0, z // 2, 0, 0)),
        ),
        out_shape=jax.ShapeDtypeStruct((16, 2, 2, 4, 8, part), BF16),
        cost_estimate=cost(2 * view.size // N_CHUNK, 4 * view.size // N_CHUNK),
    )(place, table, counts, view).reshape(64, 4, 8, part)


def combine_kernel(mods, place, arrived, *refs):
    outs, acc = refs[:-1], refs[-1]
    for k, out in enumerate(outs):
        owner = lax.rem(place[2] + k, 4)
        acc[...] = jnp.zeros_like(acc)
        for s in range(arrived.shape[0]):
            acc[mods[s]] += arrived[s, owner].astype(F32)
        out[...] = acc[...].astype(BF16)


def combine(h, mods, place, arrived):
    n, nz, rows, width = arrived.shape
    vmem = pl.BlockSpec(memory_space=pltpu.VMEM)
    smem = pl.BlockSpec(memory_space=pltpu.SMEM)
    return pl.pallas_call(
        combine_kernel,
        name=f"combine{h}",
        in_specs=[smem, smem, vmem],
        out_specs=[vmem] * nz,
        out_shape=[jax.ShapeDtypeStruct((16, rows, width), BF16)] * nz,
        scratch_shapes=[pltpu.VMEM((16, rows, width), F32)],
        cost_estimate=cost(arrived.size, 3 * arrived.size),
    )(mods, place, arrived)


def update_kernel(*refs):
    sums, outer, moment = refs[:4], refs[4], refs[5]
    outer_out, moment_out, news = refs[-3:]
    for m in range(16):
        average = sums[0][m].astype(F32)
        for more in sums[1:]:
            average += more[m].astype(F32)
        parts = []
        for layer in range(2):
            old = outer[layer, m]
            delta = old - average[layer * 4 : layer * 4 + 4]
            moved = 0.9 * moment[layer, m] + delta
            new = old - 0.7 * (delta + 0.9 * moved)
            outer_out[layer, m] = new
            moment_out[layer, m] = moved
            parts.append(new)
        news[m] = jnp.concatenate(parts, axis=0).astype(BF16)


def update(h, sums, outer, moment, before):
    part = sums[0].shape[-1]
    state = pl.BlockSpec((2, 16, 4, part), lambda g: (0, 0, 0, h))
    whole = pl.BlockSpec((16, 8, part), lambda g: (0, 0, 0))
    untouched = pl.BlockSpec(memory_space=pl.ANY)
    return pl.pallas_call(
        update_kernel,
        name=f"update{h}",
        grid=(1,),
        in_specs=[whole] * 4 + [state] * 2 + [untouched] * len(before),
        out_specs=[state, state, whole],
        out_shape=[jax.ShapeDtypeStruct(outer.shape, F32)] * 2 + [jax.ShapeDtypeStruct((16, 8, part), BF16)],
        input_output_aliases={6 + i: i for i in range(len(before))},
        cost_estimate=cost(8 * outer.size // N_CHUNK, 20 * outer.size // N_CHUNK),
    )(*sums, outer, moment, *before)


def choose_kernel(mods, place, *refs):
    news, out = refs[:-1], refs[-1]
    for k, new in enumerate(news):
        owner = lax.rem(place[2] + 4 - k, 4)
        for d in range(out.shape[0]):
            out[d, owner] = new[mods[d]]


def choose(h, mods, place, news):
    _, rows, width = news[0].shape
    vmem = pl.BlockSpec(memory_space=pltpu.VMEM)
    smem = pl.BlockSpec(memory_space=pltpu.SMEM)
    return pl.pallas_call(
        choose_kernel,
        name=f"choose{h}",
        in_specs=[smem, smem] + [vmem] * len(news),
        out_specs=vmem,
        out_shape=jax.ShapeDtypeStruct((64, 4, rows, width), BF16),
        cost_estimate=cost(0, 512 * rows * width),
    )(mods, place, *news)


def unpack_kernel(*refs):
    got, out = refs[0], refs[-1]
    for yh in range(2):
        for pair in range(8):
            rows = pl.ds(yh * 64 + pair * 8, 8)
            even = got[2 * pair, 0, yh, 0].astype(F32)
            odd = got[2 * pair + 1, 0, yh, 0].astype(F32)
            first, second = swap_halves(even, odd)
            out[0, 0, rows] = first.astype(BF16)
            out[1, 0, rows] = second.astype(BF16)


def unpack(h, got, width, before):
    part = got.shape[-1]
    view = got.reshape(16, 2, 2, 4, 8, part)
    return pl.pallas_call(
        unpack_kernel,
        name=f"unpack{h}",
        grid=(8,),
        in_specs=[pl.BlockSpec((16, 1, 2, 1, 8, part), lambda z: (0, z % 2, 0, z // 2, 0, 0))]
        + [pl.BlockSpec(memory_space=pl.ANY)] * len(before),
        out_specs=pl.BlockSpec((2, 1, 128, part), lambda z: (0, z, 0, h)),
        out_shape=jax.ShapeDtypeStruct((2, 8, 128, width), BF16),
        input_output_aliases={1: 0} if before else {},
        cost_estimate=cost(0, 8 * width * part),
    )(view, *before)


def micro_step(tokens_path, params_path):
    state = tokens_path.astype(F32)
    for layer in range(params_path.shape[0]):
        scale = lax.rsqrt(jnp.mean(state * state, axis=-1, keepdims=True) + 1e-06)
        normed = (state * scale).astype(BF16)
        mixed = jnp.dot(normed, params_path[layer], preferred_element_type=F32)
        state = state + jax.nn.gelu(mixed, approximate=False)
    return state.astype(BF16)


def in_plane(blocks):
    return lax.all_to_all(blocks, PLANE, split_axis=0, concat_axis=0, tiled=True)


def shifted(block, k):
    return lax.ppermute(block, "zh", [(i, (i + k) % 4) for i in range(4)])


def on_device(tokens, local_params, outer_params, momentum, table, counts):
    row = lax.axis_index(("yl", "x", "core")).astype(jnp.int32)
    zh = lax.axis_index("zh").astype(jnp.int32)
    col = zh * 4 + lax.axis_index(("zl", "yh")).astype(jnp.int32)
    place = jnp.stack([row, col, zh])
    mods = lax.dynamic_slice(table, (0, zh * 4), (16, 4)).reshape(64)
    params = local_params[0, 0]
    width = params.shape[-1]
    outer = outer_params.reshape(2, 16, 4, width)
    moment = momentum.reshape(2, 16, 4, width)
    hidden = micro_step(tokens[0, 0], params)
    state, whole = (), ()
    for h in range(N_CHUNK):
        arrived = in_plane(pack(h, place, table, counts, params))
        dense = combine(h, mods, place, arrived)
        sums = [dense[0]] + [shifted(dense[k], k) for k in range(1, 4)]
        *state, new = update(h, sums, outer, moment, state)
        news = [new] + [shifted(new, k) for k in range(1, 4)]
        got = in_plane(choose(h, mods, place, news))
        whole = (unpack(h, got, width, whole),)
    return (
        whole[0].reshape(local_params.shape),
        state[0].reshape(outer_params.shape),
        state[1].reshape(momentum.shape),
        hidden[None, None],
    )


def solution(mesh):
    devices = mesh.devices.reshape(2, 4, 2, 4, 2, 2)
    fine = Mesh(devices, ("yl", "x", "core", "zh", "zl", "yh"))
    row, col = ("yl", "x", "core"), ("zh", "zl", "yh")
    return jax.shard_map(
        on_device,
        mesh=fine,
        in_specs=(
            P(row, col, None, None),
            P(row, col, None, None, None),
            P(None, None, col, row, None, None),
            P(None, None, col, row, None, None),
            P(),
            P(),
        ),
        out_specs=(
            P(row, col, None, None, None),
            P(None, None, col, row, None, None),
            P(None, None, col, row, None, None),
            P(row, col, None, None),
        ),
        check_vma=False,
    )
```

```python
import functools

import jax
import jax.numpy as jnp
from jax import lax
from jax.experimental import pallas as pl
from jax.experimental.pallas import tpu as pltpu
from jax.sharding import Mesh
from jax.sharding import PartitionSpec as P

PLANE = ("yl", "x", "core", "zl", "yh")
SHIFTS = (2, 1, 3, 0)
F32 = jnp.float32
BF16 = jnp.bfloat16


LARGE = pltpu.CompilerParams(vmem_limit_bytes=61 * 2**20)
SMALL = pltpu.CompilerParams(vmem_limit_bytes=16 * 2**20)


def cost(flops, bytes_accessed):
    return pl.CostEstimate(flops=flops, bytes_accessed=bytes_accessed, transcendentals=0)


def low_half(shape):
    return lax.broadcasted_iota(jnp.int32, shape, len(shape) - 2) < 4


def swap_halves(first, second):
    mask = low_half(first.shape)
    axis = len(first.shape) - 2
    return (
        jnp.where(mask, first, pltpu.roll(second, 4, axis)),
        jnp.where(mask, pltpu.roll(first, 4, axis), second),
    )


def pack_kernel(place, table, counts, params, out, held, done, sem_in, sem_out):
    loads = [pltpu.make_async_copy(params.at[:, z], held.at[:, z], sem_in.at[z]) for z in range(8)]
    for load in loads:
        load.start()
    ids = table[...]
    tokens = counts[...].astype(F32)
    here = (lax.broadcasted_iota(jnp.int32, ids.shape, 0) == place[0]) & (
        lax.broadcasted_iota(jnp.int32, ids.shape, 1) == place[1]
    )
    module = jnp.sum(jnp.where(here, ids, 0).astype(F32))
    total = jnp.sum(jnp.where(ids.astype(F32) == module, tokens, 0.0), keepdims=True)
    mine = jnp.sum(jnp.where(here, tokens, 0.0), keepdims=True)
    share = jnp.broadcast_to(mine / total, (8, held.shape[-1]))
    stores = []
    for z in range(8):
        loads[z].wait()
        for yh in range(2):
            for pair in range(8):
                rows = pl.ds(yh * 64 + pair * 8, 8)
                first = held[0, z, rows].astype(F32) * share
                second = held[1, z, rows].astype(F32) * share
                even, odd = swap_halves(first, second)
                done[z, 2 * pair, yh] = even.astype(BF16)
                done[z, 2 * pair + 1, yh] = odd.astype(BF16)
        stores.append(pltpu.make_async_copy(done.at[z], out.at[:, z % 2, :, z // 2], sem_out.at[z]))
        stores[-1].start()
    for store in stores:
        store.wait()


def pack(place, table, counts, params):
    layers, width = params.shape[0], params.shape[-1]
    view = params.reshape(layers, 8, 128, width)
    vmem = pl.BlockSpec(memory_space=pltpu.VMEM)
    return pl.pallas_call(
        pack_kernel,
        name="pack",
        compiler_params=LARGE,
        in_specs=[pl.BlockSpec(memory_space=pltpu.SMEM), vmem, vmem, pl.BlockSpec(memory_space=pltpu.HBM)],
        out_specs=pl.BlockSpec(memory_space=pltpu.HBM),
        out_shape=jax.ShapeDtypeStruct((16, 2, 2, 4, 8, width), BF16),
        scratch_shapes=[
            pltpu.VMEM(view.shape, BF16),
            pltpu.VMEM((8, 16, 2, 8, width), BF16),
            pltpu.SemaphoreType.DMA((8,)),
            pltpu.SemaphoreType.DMA((8,)),
        ],
        cost_estimate=cost(2 * view.size, 4 * view.size),
    )(place, table, counts, view).reshape(64, 4, 8, width)


def combine_kernel(k, mods, place, arrived, out, held, acc, sems):
    owner = lax.rem(place[2] + k, 4)
    loads = [
        pltpu.make_async_copy(arrived.at[pl.ds(g * 16, 16), owner], held.at[pl.ds(g * 16, 16)], sems.at[g])
        for g in range(4)
    ]
    for load in loads:
        load.start()
    acc[...] = jnp.zeros_like(acc)
    for g, load in enumerate(loads):
        load.wait()
        for s in range(g * 16, g * 16 + 16):
            acc[mods[s]] += held[s].astype(F32)
    out[...] = acc[...].astype(BF16)


def combine(k, mods, place, arrived):
    n, nz, rows, width = arrived.shape
    smem = pl.BlockSpec(memory_space=pltpu.SMEM)
    return pl.pallas_call(
        functools.partial(combine_kernel, k),
        compiler_params=LARGE,
        in_specs=[smem, smem, pl.BlockSpec(memory_space=pltpu.HBM)],
        out_specs=pl.BlockSpec(memory_space=pltpu.VMEM),
        out_shape=jax.ShapeDtypeStruct((16, rows, width), BF16),
        scratch_shapes=[
            pltpu.VMEM((n, rows, width), BF16),
            pltpu.VMEM((16, rows, width), F32),
            pltpu.SemaphoreType.DMA((4,)),
        ],
        cost_estimate=cost(arrived.size // nz, 3 * arrived.size // nz),
    )(mods, place, arrived)


def update_kernel(*refs):
    sums, outer, moment = refs[:4], refs[4], refs[5]
    outer_out, moment_out, news = refs[-3:]
    for m in range(16):
        average = sums[0][m].astype(F32)
        for more in sums[1:]:
            average += more[m].astype(F32)
        parts = []
        for layer in range(2):
            old = outer[layer, m]
            delta = old - average[layer * 4 : layer * 4 + 4]
            moved = 0.9 * moment[layer, m] + delta
            new = old - 0.7 * (delta + 0.9 * moved)
            outer_out[layer, m] = new
            moment_out[layer, m] = moved
            parts.append(new)
        news[m] = jnp.concatenate(parts, axis=0).astype(BF16)


def update(sums, outer, moment):
    width = outer.shape[-1]
    part = width // 2
    state = pl.BlockSpec((2, 16, 4, part), lambda h: (0, 0, 0, h))
    whole = pl.BlockSpec((16, 8, part), lambda h: (0, 0, h))
    return pl.pallas_call(
        update_kernel,
        name="update",
        compiler_params=SMALL,
        grid=(2,),
        in_specs=[whole] * 4 + [state] * 2,
        out_specs=[state, state, whole],
        out_shape=[jax.ShapeDtypeStruct(outer.shape, F32)] * 2 + [jax.ShapeDtypeStruct((16, 8, width), BF16)],
        cost_estimate=cost(8 * outer.size, 20 * outer.size),
    )(*sums, outer, moment)


def choose_kernel(shifts, mods, place, *refs):
    news, (out, held, sems) = refs[: len(shifts)], refs[-3:]
    copies = []
    for i, k in enumerate(shifts):
        owner = lax.rem(place[2] + 4 - k, 4)
        for g in range(2):
            part = pl.ds(g * 32, 32)
            for d in range(g * 32, g * 32 + 32):
                held[i, d] = news[i][mods[d]]
            copies.append(pltpu.make_async_copy(held.at[i, part], out.at[part, owner], sems.at[i, g]))
            copies[-1].start()
    for copy in copies:
        copy.wait()


def choose(shifts, mods, place, news, before):
    _, rows, width = news[0].shape
    n = len(shifts)
    vmem = pl.BlockSpec(memory_space=pltpu.VMEM)
    smem = pl.BlockSpec(memory_space=pltpu.SMEM)
    hbm = pl.BlockSpec(memory_space=pltpu.HBM)
    return pl.pallas_call(
        functools.partial(choose_kernel, shifts),
        name="choose",
        compiler_params=LARGE,
        in_specs=[smem, smem] + [vmem] * n + [hbm] * len(before),
        out_specs=hbm,
        out_shape=jax.ShapeDtypeStruct((64, 4, rows, width), BF16),
        scratch_shapes=[pltpu.VMEM((n, 64, rows, width), BF16), pltpu.SemaphoreType.DMA((n, 2))],
        input_output_aliases={2 + n: 0} if before else {},
        cost_estimate=cost(0, 160 * n * rows * width),
    )(mods, place, *news, *before)


def unpack_kernel(got, out, held, done, sem_in, sem_out):
    loads = [pltpu.make_async_copy(got.at[:, z % 2, :, z // 2], held.at[z], sem_in.at[z]) for z in range(8)]
    for load in loads:
        load.start()
    stores = []
    for z in range(8):
        loads[z].wait()
        for yh in range(2):
            for pair in range(8):
                rows = pl.ds(yh * 64 + pair * 8, 8)
                even = held[z, 2 * pair, yh].astype(F32)
                odd = held[z, 2 * pair + 1, yh].astype(F32)
                first, second = swap_halves(even, odd)
                done[0, z, rows] = first.astype(BF16)
                done[1, z, rows] = second.astype(BF16)
        stores.append(pltpu.make_async_copy(done.at[:, z], out.at[:, z], sem_out.at[z]))
        stores[-1].start()
    for store in stores:
        store.wait()


def unpack(got):
    width = got.shape[-1]
    hbm = pl.BlockSpec(memory_space=pltpu.HBM)
    shape = (2, 8, 128, width)
    return pl.pallas_call(
        unpack_kernel,
        name="unpack",
        compiler_params=SMALL,
        in_specs=[hbm],
        out_specs=hbm,
        out_shape=jax.ShapeDtypeStruct(shape, BF16),
        scratch_shapes=[
            pltpu.VMEM((8, 16, 2, 8, width), BF16),
            pltpu.VMEM(shape, BF16),
            pltpu.SemaphoreType.DMA((8,)),
            pltpu.SemaphoreType.DMA((8,)),
        ],
        cost_estimate=cost(0, 8 * width * width),
    )(got.reshape(16, 2, 2, 4, 8, width))


def micro_step(tokens_path, params_path):
    state = tokens_path.astype(F32)
    for layer in range(params_path.shape[0]):
        scale = lax.rsqrt(jnp.mean(state * state, axis=-1, keepdims=True) + 1e-06)
        normed = (state * scale).astype(BF16)
        mixed = jnp.dot(normed, params_path[layer], preferred_element_type=F32)
        state = state + jax.nn.gelu(mixed, approximate=False)
    return state.astype(BF16)


def in_plane(blocks):
    return lax.all_to_all(blocks, PLANE, split_axis=0, concat_axis=0, tiled=True)


def shifted(block, k):
    return block if k == 0 else lax.ppermute(block, "zh", [(i, (i + k) % 4) for i in range(4)])


def body(tokens, local_params, outer_params, momentum, table, counts):
    row = lax.axis_index(("yl", "x", "core")).astype(jnp.int32)
    zh = lax.axis_index("zh").astype(jnp.int32)
    col = zh * 4 + lax.axis_index(("zl", "yh")).astype(jnp.int32)
    place = jnp.stack([row, col, zh])
    mods = lax.dynamic_slice(table, (0, zh * 4), (16, 4)).reshape(64)
    params = local_params[0, 0]
    width = params.shape[-1]
    outer = outer_params.reshape(2, 16, 4, width)
    moment = momentum.reshape(2, 16, 4, width)
    hidden = micro_step(tokens[0, 0], params)
    arrived = in_plane(pack(place, table, counts, params))
    sums = []
    for k in SHIFTS:
        dense = combine(k, mods, place, arrived)
        sums.append(shifted(dense, k))
    outer_new, moment_new, new = update(sums, outer, moment)
    news = []
    for k in SHIFTS:
        news.append(shifted(new, k))
    chosen = choose((0,), mods, place, news[3:], ())
    chosen = choose(SHIFTS[:3], mods, place, news[:3], (chosen,))
    got = in_plane(chosen)
    return (
        unpack(got).reshape(local_params.shape),
        outer_new.reshape(outer_params.shape),
        moment_new.reshape(momentum.shape),
        hidden[None, None],
    )


def solution(mesh):
    devices = mesh.devices.reshape(2, 4, 2, 4, 2, 2)
    fine = Mesh(devices, ("yl", "x", "core", "zh", "zl", "yh"))
    row, col = ("yl", "x", "core"), ("zh", "zl", "yh")
    return jax.shard_map(
        body,
        mesh=fine,
        in_specs=(
            P(row, col, None, None),
            P(row, col, None, None, None),
            P(None, None, col, row, None, None),
            P(None, None, col, row, None, None),
            P(),
            P(),
        ),
        out_specs=(
            P(row, col, None, None, None),
            P(None, None, col, row, None, None),
            P(None, None, col, row, None, None),
            P(row, col, None, None),
        ),
        check_vma=False,
    )
```

```python
import functools

import jax
import jax.numpy as jnp
from jax import lax
from jax.experimental import pallas as pl
from jax.experimental.pallas import tpu as pltpu
from jax.sharding import Mesh
from jax.sharding import PartitionSpec as P

PLANE = ("yl", "x", "core", "zl", "yh")
SHIFTS = (1, 3, 2, 0)
N_CHUNK = 2


F32 = jnp.float32
BF16 = jnp.bfloat16


LARGE = pltpu.CompilerParams(vmem_limit_bytes=60 * 2**20)
SMALL = pltpu.CompilerParams(vmem_limit_bytes=16 * 2**20)


def cost(flops, bytes_accessed):
    return pl.CostEstimate(flops=flops, bytes_accessed=bytes_accessed, transcendentals=0)


def my_row():
    return lax.axis_index(("yl", "x", "core")).astype(jnp.int32)


def my_col():
    return lax.axis_index(("zh", "zl", "yh")).astype(jnp.int32)


def low_half(shape):
    return lax.broadcasted_iota(jnp.int32, shape, len(shape) - 2) < 4


def swap_halves(first, second):
    mask = low_half(first.shape)
    axis = len(first.shape) - 2
    return (
        jnp.where(mask, first, pltpu.roll(second, 4, axis)),
        jnp.where(mask, pltpu.roll(first, 4, axis), second),
    )


def pack_kernel(table, counts, params, out, held, done, sem_in, sem_out):
    loads = [pltpu.make_async_copy(params.at[:, z], held.at[:, z], sem_in.at[z]) for z in range(8)]
    for load in loads:
        load.start()
    ids = table[...]
    tokens = counts[...].astype(F32)
    here = (lax.broadcasted_iota(jnp.int32, ids.shape, 0) == my_row()) & (
        lax.broadcasted_iota(jnp.int32, ids.shape, 1) == my_col()
    )
    module = jnp.sum(jnp.where(here, ids, 0).astype(F32))
    total = jnp.sum(jnp.where(ids.astype(F32) == module, tokens, 0.0), keepdims=True)
    mine = jnp.sum(jnp.where(here, tokens, 0.0), keepdims=True)
    share = jnp.broadcast_to(mine / total, (8, held.shape[-1]))
    stores = []
    for z in range(8):
        loads[z].wait()
        for yh in range(2):
            for pair in range(8):
                rows = pl.ds(yh * 64 + pair * 8, 8)
                first = held[0, z, rows].astype(F32) * share
                second = held[1, z, rows].astype(F32) * share
                even, odd = swap_halves(first, second)
                done[z, 2 * pair, yh] = even.astype(BF16)
                done[z, 2 * pair + 1, yh] = odd.astype(BF16)
        stores.append(pltpu.make_async_copy(done.at[z], out.at[:, z % 2, :, z // 2], sem_out.at[z]))
        stores[-1].start()
    for store in stores:
        store.wait()


def pack(table, counts, params):
    layers, width = params.shape[0], params.shape[-1]
    view = params.reshape(layers, 8, 128, width)
    vmem = pl.BlockSpec(memory_space=pltpu.VMEM)
    return pl.pallas_call(
        pack_kernel,
        name="pack",
        compiler_params=LARGE,
        in_specs=[vmem, vmem, pl.BlockSpec(memory_space=pltpu.HBM)],
        out_specs=pl.BlockSpec(memory_space=pltpu.HBM),
        out_shape=jax.ShapeDtypeStruct((16, 2, 2, 4, 8, width), BF16),
        scratch_shapes=[
            pltpu.VMEM(view.shape, BF16),
            pltpu.VMEM((8, 16, 2, 8, width), BF16),
            pltpu.SemaphoreType.DMA((8,)),
            pltpu.SemaphoreType.DMA((8,)),
        ],
        cost_estimate=cost(2 * view.size, 4 * view.size),
    )(table, counts, view).reshape(64, 4, 8, width)


def combine_kernel(h, k, mods_in, arrived, out, held, acc, mods, sems):
    owner = lax.rem(lax.axis_index("zh").astype(jnp.int32) + k, 4)
    cols = pl.ds(h * held.shape[-1], held.shape[-1])
    fetch = pltpu.make_async_copy(mods_in, mods, sems.at[4])
    fetch.start()
    parts = [pl.ds(g * 16, 16) for g in range(4)]
    loads = [
        pltpu.make_async_copy(arrived.at[part, owner, :, cols], held.at[part], sems.at[g])
        for g, part in enumerate(parts)
    ]
    for load in loads:
        load.start()
    acc[...] = jnp.zeros_like(acc)
    fetch.wait()
    for g, load in enumerate(loads):
        load.wait()
        for first in range(g * 16, g * 16 + 16, 4):
            slots = [mods[first + c] for c in range(4)]
            added = [acc[slot] + held[first + c].astype(F32) for c, slot in enumerate(slots)]
            for slot, value in zip(slots, added):
                acc[slot] = value
    out[...] = acc[...].astype(BF16)


def combine(h, k, mods, arrived):
    n, _, rows, width = arrived.shape
    width = width // N_CHUNK
    hbm = pl.BlockSpec(memory_space=pltpu.HBM)
    return pl.pallas_call(
        functools.partial(combine_kernel, h, k),
        name="combine",
        compiler_params=SMALL,
        in_specs=[hbm, hbm],
        out_specs=pl.BlockSpec(memory_space=pltpu.VMEM),
        out_shape=jax.ShapeDtypeStruct((16, rows, width), BF16),
        scratch_shapes=[
            pltpu.VMEM((n, rows, width), BF16),
            pltpu.VMEM((16, rows, width), F32),
            pltpu.SMEM((n,), jnp.int32),
            pltpu.SemaphoreType.DMA((5,)),
        ],
        cost_estimate=cost(arrived.size // 8, 3 * arrived.size // 8),
    )(mods, arrived)


def update_kernel(*refs):
    sums, outer, moment = refs[:4], refs[4], refs[5]
    outer_out, moment_out, news = refs[-3:]
    for m in range(16):
        average = sums[0][m].astype(F32)
        for more in sums[1:]:
            average += more[m].astype(F32)
        parts = []
        for layer in range(2):
            old = outer[layer, m]
            delta = old - average[layer * 4 : layer * 4 + 4]
            moved = 0.9 * moment[layer, m] + delta
            new = old - 0.7 * (delta + 0.9 * moved)
            outer_out[layer, m] = new
            moment_out[layer, m] = moved
            parts.append(new)
        news[m] = jnp.concatenate(parts, axis=0).astype(BF16)


def update(h, sums, outer, moment, before):
    part = sums[0].shape[-1]
    state = pl.BlockSpec((2, 16, 4, part), lambda g: (0, 0, 0, h))
    whole = pl.BlockSpec((16, 8, part), lambda g: (0, 0, 0))
    return pl.pallas_call(
        update_kernel,
        name="update",
        compiler_params=SMALL,
        grid=(1,),
        in_specs=[whole] * 4 + [state] * 2 + [pl.BlockSpec(memory_space=pl.ANY)] * len(before),
        out_specs=[state, state, whole],
        out_shape=[jax.ShapeDtypeStruct(outer.shape, F32)] * 2 + [jax.ShapeDtypeStruct((16, 8, part), BF16)],
        input_output_aliases={6 + i: i for i in range(len(before))},
        cost_estimate=cost(4 * outer.size, 10 * outer.size),
    )(*sums, outer, moment, *before)


def choose_kernel(h, shifts, mods, *refs):
    news, (out, held, sems) = refs[: len(shifts)], refs[-3:]
    cols = pl.ds(h * held.shape[-1], held.shape[-1])
    copies = []
    for i, k in enumerate(shifts):
        owner = lax.rem(lax.axis_index("zh").astype(jnp.int32) + 4 - k, 4)
        for g in range(2):
            part = pl.ds(g * 32, 32)
            for d in range(g * 32, g * 32 + 32):
                held[i, d] = news[i][mods[d]]
            copies.append(pltpu.make_async_copy(held.at[i, part], out.at[part, owner, :, cols], sems.at[i, g]))
            copies[-1].start()
    for copy in copies:
        copy.wait()


def choose(h, shifts, mods, news, before):
    _, rows, part = news[0].shape
    n = len(shifts)
    vmem = pl.BlockSpec(memory_space=pltpu.VMEM)
    smem = pl.BlockSpec(memory_space=pltpu.SMEM)
    hbm = pl.BlockSpec(memory_space=pltpu.HBM)
    return pl.pallas_call(
        functools.partial(choose_kernel, h, shifts),
        name="choose",
        compiler_params=LARGE,
        in_specs=[smem] + [vmem] * n + [hbm] * len(before),
        out_specs=hbm,
        out_shape=jax.ShapeDtypeStruct((64, 4, rows, part * N_CHUNK), BF16),
        scratch_shapes=[pltpu.VMEM((n, 64, rows, part), BF16), pltpu.SemaphoreType.DMA((n, 2))],
        input_output_aliases={1 + n: 0} if before else {},
        cost_estimate=cost(0, 160 * n * rows * part),
    )(mods, *news, *before)


def unpack_kernel(got, out, held, done, sem_in, sem_out):
    loads = [pltpu.make_async_copy(got.at[:, z % 2, :, z // 2], held.at[z], sem_in.at[z]) for z in range(8)]
    for load in loads:
        load.start()
    stores = []
    for z in range(8):
        loads[z].wait()
        for yh in range(2):
            for pair in range(8):
                rows = pl.ds(yh * 64 + pair * 8, 8)
                even = held[z, 2 * pair, yh].astype(F32)
                odd = held[z, 2 * pair + 1, yh].astype(F32)
                first, second = swap_halves(even, odd)
                done[0, z, rows] = first.astype(BF16)
                done[1, z, rows] = second.astype(BF16)
        stores.append(pltpu.make_async_copy(done.at[:, z], out.at[:, z], sem_out.at[z]))
        stores[-1].start()
    for store in stores:
        store.wait()


def unpack(got):
    width = got.shape[-1]
    hbm = pl.BlockSpec(memory_space=pltpu.HBM)
    shape = (2, 8, 128, width)
    return pl.pallas_call(
        unpack_kernel,
        name="unpack",
        compiler_params=SMALL,
        in_specs=[hbm],
        out_specs=hbm,
        out_shape=jax.ShapeDtypeStruct(shape, BF16),
        scratch_shapes=[
            pltpu.VMEM((8, 16, 2, 8, width), BF16),
            pltpu.VMEM(shape, BF16),
            pltpu.SemaphoreType.DMA((8,)),
            pltpu.SemaphoreType.DMA((8,)),
        ],
        cost_estimate=cost(0, 8 * width * width),
    )(got.reshape(16, 2, 2, 4, 8, width))


def micro_step(tokens_path, params_path):
    state = tokens_path.astype(F32)
    for layer in range(params_path.shape[0]):
        scale = lax.rsqrt(jnp.mean(state * state, axis=-1, keepdims=True) + 1e-06)
        normed = (state * scale).astype(BF16)
        mixed = jnp.dot(normed, params_path[layer], preferred_element_type=F32)
        state = state + jax.nn.gelu(mixed, approximate=False)
    return state.astype(BF16)


def in_plane(blocks):
    return lax.all_to_all(blocks, PLANE, split_axis=0, concat_axis=0, tiled=True)


def shifted(block, k):
    return block if k == 0 else lax.ppermute(block, "zh", [(i, (i + k) % 4) for i in range(4)])


def body(tokens, local_params, outer_params, momentum, table, counts):
    zh = lax.axis_index("zh").astype(jnp.int32)
    mods = lax.dynamic_slice(table, (0, zh * 4), (16, 4)).reshape(64)
    params = local_params[0, 0]
    width = params.shape[-1]
    outer = outer_params.reshape(2, 16, 4, width)
    moment = momentum.reshape(2, 16, 4, width)
    hidden = micro_step(tokens[0, 0], params)
    arrived = in_plane(pack(table, counts, params))
    sums = {}
    for h in range(N_CHUNK):
        for k in SHIFTS:
            dense = combine(h, k, mods, arrived)
            sums[h, k] = shifted(dense, k)
    state, news = (), {}
    for h in range(N_CHUNK):
        *state, new = update(h, [sums[h, k] for k in SHIFTS], outer, moment, state)
        for k in SHIFTS:
            news[h, k] = shifted(new, k)
    outer_new, moment_new = state
    chosen = choose(0, SHIFTS, mods, [news[0, k] for k in SHIFTS], ())
    chosen = choose(1, (0,), mods, [news[1, 0]], (chosen,))
    chosen = choose(1, SHIFTS[:2], mods, [news[1, k] for k in SHIFTS[:2]], (chosen,))
    chosen = choose(1, SHIFTS[2:3], mods, [news[1, SHIFTS[2]]], (chosen,))
    got = in_plane(chosen)
    return (
        unpack(got).reshape(local_params.shape),
        outer_new.reshape(outer_params.shape),
        moment_new.reshape(momentum.shape),
        hidden[None, None],
    )


def solution(mesh):
    devices = mesh.devices.reshape(2, 4, 2, 4, 2, 2)
    fine = Mesh(devices, ("yl", "x", "core", "zh", "zl", "yh"))
    row, col = ("yl", "x", "core"), ("zh", "zl", "yh")
    return jax.shard_map(
        body,
        mesh=fine,
        in_specs=(
            P(row, col, None, None),
            P(row, col, None, None, None),
            P(None, None, col, row, None, None),
            P(None, None, col, row, None, None),
            P(),
            P(),
        ),
        out_specs=(
            P(row, col, None, None, None),
            P(None, None, col, row, None, None),
            P(None, None, col, row, None, None),
            P(row, col, None, None),
        ),
        check_vma=False,
    )
```
